32 devices in a mesh: gx: 2 (over x), gy: 4 (over y, core), gz: 4 (over z).
Axes of the slice: x: 2, y: 2, z: 4, core: 2. Of those that a mesh axis runs over, the one named last changes fastest.
Arguments:
- estimate: float32 [48, 128, 512], P('gx', 'gy', 'gz'), may hold values from 0.03 to 11, as said below
- view_images: float32 [4, 48, 128, 512], P(None, 'gx', 'gy', 'gz'), may hold values from 0.015 to 21, as said below
- psf_taps: int32 [4, 3, 31], replicated, may hold values from 1 to 64
- view_weights: int32 [4], replicated, may hold values from 1 to 4
Outputs:
- deconvolved: float32 [48, 128, 512], P('gx', 'gy', 'gz')
- misfit: float32 [2, 4], replicated
The draws below stay inside these ranges and needn't reach their ends.
Inputs may be any that keep to these rules, and one draw needn't show every extreme that they name: `estimate`: positive. `view_images`: positive.
All inputs are finite; a program needn't handle non-finite values.
Results may differ from the reference program's by a relative error of at most 0.0001.
Values sent between devices are 32-bit elements; how exact they have to be, the bound alone decides.
A program may use at most 128 MiB of HBM per device.

```python
import jax
import jax.numpy as jnp
from jax import lax

VIEWS = 4
TAPS = 31
ITERS = 2
NX = 48
NY = 128
NZ = 512


def ramp_profile(rising):
    first = (jnp.arange(NX, dtype=jnp.float32) + 0.5) / NX
    second = (jnp.arange(NY, dtype=jnp.float32) + 0.5) / NY
    third = (jnp.arange(NZ, dtype=jnp.float32) + 0.5) / NZ
    if rising:
        return (0.5 + first)[:, None, None] * (0.5 + second)[None, :, None] * (0.5 + third)[None, None, :]
    return (1.5 - first)[:, None, None] * (1.5 - second)[None, :, None] * (1.5 - third)[None, None, :]


def draw_view_images(key, part):
    inner = jax.random.fold_in(key, 11)
    profile = ramp_profile(True)[None]
    rough = jax.random.uniform(inner, (VIEWS, NX, NY, NZ), jnp.float32, 0.5, 2.0)
    return (profile * rough).astype(jnp.float32)


def draw_estimate(key, part):
    inner = jax.random.fold_in(key, 23)
    profile = ramp_profile(False)
    rough = jax.random.uniform(inner, (NX, NY, NZ), jnp.float32, 0.5, 1.5)
    return (profile * rough).astype(jnp.float32)


def set_ends(entries, stream_key, low, largest):
    longest = entries.shape.index(max(entries.shape))
    spots = []
    for shift in (0, 1):
        where = [jax.random.randint(jax.random.fold_in(stream_key, axis), (), 0, length) for axis, length in enumerate(entries.shape)]
        where[longest] = (where[longest] + shift) % entries.shape[longest]
        spots.append(tuple(where))
    return entries.at[spots[0]].set(low).at[spots[1]].set(largest)


def setup_inputs(seed: int = 0) -> dict:
    arg_keys = jax.random.split(jax.random.key(seed), 5)
    return {
        "estimate": draw_estimate(jax.random.fold_in(arg_keys[4], 71), 0),
        "view_images": draw_view_images(jax.random.fold_in(arg_keys[4], 71), 0),
        "psf_taps": set_ends(jax.random.randint(arg_keys[2], (VIEWS, 3, TAPS), 1, 65), jax.random.fold_in(arg_keys[2], 1), 1, 64).astype(jnp.int32),
        "view_weights": set_ends(jax.random.randint(arg_keys[3], (VIEWS,), 1, 5), jax.random.fold_in(arg_keys[3], 1), 1, 4).astype(jnp.int32),
    }


def convolve_axis(volume, kernel, axis_dim):
    moved = jnp.moveaxis(volume, axis_dim, -1)
    saved_shape = moved.shape
    flattened = moved.reshape(-1, 1, saved_shape[-1])
    reach = (TAPS - 1) // 2
    convolved = lax.conv_general_dilated(flattened, kernel.reshape(1, 1, -1), (1,), [(reach, reach)], dimension_numbers=("NCH", "OIH", "NCH"), precision=lax.Precision.HIGHEST)
    return jnp.moveaxis(convolved.reshape(saved_shape), -1, axis_dim)


def reference(estimate, view_images, psf_taps, view_weights):
    kernels = psf_taps.astype(jnp.float32) / 256.0
    flipped = kernels[:, :, ::-1]
    tap_sums = jnp.sum(kernels, axis=2)
    weight_float = view_weights.astype(jnp.float32)
    normalizer = jnp.sum(weight_float * jnp.prod(tap_sums, axis=1))
    data_total = jnp.sum(view_images, axis=(1, 2, 3))
    data_square = jnp.sum(view_images * view_images, axis=(1, 2, 3))
    misfits = []
    for iteration in range(ITERS):
        correction = jnp.zeros_like(estimate)
        row = []
        for view_index in range(VIEWS):
            blurred = convolve_axis(estimate, kernels[view_index, 0], 0)
            blurred = convolve_axis(blurred, kernels[view_index, 1], 1)
            blurred = convolve_axis(blurred, kernels[view_index, 2], 2)
            flux_scale = data_total[view_index] / jnp.sum(blurred)
            scaled = flux_scale * blurred
            difference = view_images[view_index] - scaled
            row.append(jnp.sum(difference * difference) / data_square[view_index])
            quotient = view_images[view_index] / scaled
            backed = convolve_axis(quotient, flipped[view_index, 0], 0)
            backed = convolve_axis(backed, flipped[view_index, 1], 1)
            backed = convolve_axis(backed, flipped[view_index, 2], 2)
            correction = correction + weight_float[view_index] * backed
        estimate = estimate * (correction / normalizer)
        misfits.append(jnp.stack(row))
    return estimate, jnp.stack(misfits)
```

```python
import functools

import jax
import jax.numpy as jnp
from jax import lax
from jax.experimental import pallas as pl
from jax.experimental.pallas import tpu as pltpu
from jax.sharding import PartitionSpec as P

TAPS = 31
ITERS = 2
REACH = 15
PAD = 16
LANES = 128
MESH = pl.DeviceIdType.MESH
AXES = ("gx", "gy", "gz")
F32 = jnp.float32
BF16 = jnp.bfloat16
STATS = 5


def halves(value, axis):
    high = value.astype(BF16).astype(F32)
    return jnp.concatenate([high, value - high], axis=axis).astype(BF16)


def dot(left, right):
    return jnp.dot(left, right, preferred_element_type=F32)


def dot_nt(left, right):
    return lax.dot_general(left, right, (((1,), (1,)), ((), ())), preferred_element_type=F32)


def dot_tn(left, right):
    return lax.dot_general(left, right, (((0,), (0,)), ((), ())), preferred_element_type=F32)


def iota(shape, dim):
    return lax.broadcasted_iota(jnp.int32, shape, dim)


class Shift:
    def __init__(self, axis, count, step, source, target, send_sem, recv_sem, swap=False):
        me = lax.axis_index(axis)
        if swap:
            self.sends = self.receives = None
            goal = 1 - me
        else:
            self.sends = (me + step >= 0) & (me + step < count)
            self.receives = (me - step >= 0) & (me - step < count)
            goal = me + step
        self.copy = pltpu.make_async_remote_copy(
            src_ref=source, dst_ref=target, send_sem=send_sem, recv_sem=recv_sem,
            device_id={axis: goal}, device_id_type=MESH,
        )

    def when(self, condition, action):
        if condition is None:
            action()
        else:
            pl.when(condition)(action)

    def start(self):
        self.when(self.sends, self.copy.start)

    def wait_recv(self):
        self.when(self.receives, self.copy.wait_recv)

    def wait_send(self):
        self.when(self.sends, self.copy.wait_send)


def kernel(sizes, taps_ref, weights_ref, est_ref, images_ref, out_ref, misfit_ref,
           img, eo, eh, fo, fh, quo, uo, uh, co, ch, ts, tr, bs, br, ry, rx, yr, xr, stats, ar, ar_own, scale,
           kx, kxb, ky, kyb, kz, kzh, kzb, img_sem, send, recv, ar_send, ar_recv):
    counts, (views, nx, ny, nz) = sizes
    xs = eo.shape[2]
    ys = ny + 2 * PAD
    fstride = fo.shape[0] // (views * nx)
    ustride = uo.shape[0] // ys
    chunk = 8
    rows = chunk * ny
    blocks = nx // chunk
    flat = ys * xs
    pieces = flat // LANES
    swap = counts[0] == 2
    mx, my, mz = (lax.axis_index(a) for a in AXES)

    image_copy = pltpu.make_async_copy(images_ref, img, img_sem)
    image_copy.start()

    barrier = pltpu.get_barrier_semaphore()
    greeted = 0
    for axis, count, me in zip(AXES, counts, (mx, my, mz)):
        for p in range(1, count):
            pl.semaphore_signal(barrier, inc=1, device_id={axis: lax.rem(me + p, count)}, device_id_type=MESH)
            greeted += 1

    for y in range(ny):
        eo[0, PAD + y, 0:nx, :] = est_ref[pl.ds(y, nx, stride=ny), :]

    pl.semaphore_wait(barrier, greeted)

    own_y = pl.ds(PAD, ny)
    face = pl.multiple_of((1 - mx) * (nx - PAD), 8) if swap else None

    def x_gather(it):
        if swap:
            return [Shift("gx", 2, 1, eo.at[it, own_y, pl.ds(face, PAD), :], xr.at[it, 0],
                          send.at[it, 0], recv.at[it, 0], swap=True)]
        return [
            Shift("gx", counts[0], 1, eo.at[it, own_y, pl.ds(nx - PAD, PAD), :],
                  xr.at[it, 0], send.at[it, 0], recv.at[it, 0]),
            Shift("gx", counts[0], -1, eo.at[it, own_y, pl.ds(0, PAD), :],
                  xr.at[it, 1], send.at[it, 1], recv.at[it, 1]),
        ]

    def y_gather(it):
        return [
            Shift("gy", counts[1], 1, eo.at[it, pl.ds(ny, PAD)], yr.at[it, 0],
                  send.at[it, 2], recv.at[it, 2]),
            Shift("gy", counts[1], -1, eo.at[it, pl.ds(PAD, PAD)], yr.at[it, 1],
                  send.at[it, 3], recv.at[it, 3]),
        ]

    def z_pair(it, source, target, first):
        return [
            Shift("gz", counts[2], 1, source.at[it, pl.ds(PAD, PAD)], target.at[it, pl.ds(0, PAD)],
                  send.at[it, first], recv.at[it, first]),
            Shift("gz", counts[2], -1, source.at[it, pl.ds(0, PAD)], target.at[it, pl.ds(PAD, PAD)],
                  send.at[it, first + 1], recv.at[it, first + 1]),
        ]

    def y_reduce(it):
        return [
            Shift("gy", counts[1], 1, co.at[it, pl.ds(PAD + ny, PAD)], ry.at[it, 0],
                  send.at[it, 8], recv.at[it, 8]),
            Shift("gy", counts[1], -1, co.at[it, pl.ds(0, PAD)], ry.at[it, 1],
                  send.at[it, 9], recv.at[it, 9]),
        ]

    def x_reduce(it):
        if swap:
            return [Shift("gx", 2, 1, co.at[it, own_y, pl.ds(nx, PAD), :], rx.at[it, 0],
                          send.at[it, 10], recv.at[it, 10], swap=True)]
        return [
            Shift("gx", counts[0], 1, co.at[it, own_y, pl.ds(nx + PAD, PAD), :], rx.at[it, 0],
                  send.at[it, 10], recv.at[it, 10]),
            Shift("gx", counts[0], -1, co.at[it, own_y, pl.ds(nx, PAD), :], rx.at[it, 1],
                  send.at[it, 11], recv.at[it, 11]),
        ]

    def start(copies):
        for c in copies:
            c.start()
        return copies

    def arrive(copies):
        for c in copies:
            c.wait_recv()
            c.wait_send()

    gathers = start(x_gather(0))

    def edges():
        def clear(condition, ref, index):
            @pl.when(condition)
            def _():
                ref[index] = jnp.zeros(ref.at[index].shape, F32)
        for it in range(ITERS):
            clear(my == 0, yr, (it, 0))
            clear(my == counts[1] - 1, yr, (it, 1))
            clear(my == 0, ry, (it, 0))
            clear(my == counts[1] - 1, ry, (it, 1))
            for ref in (tr, br):
                clear(mz == 0, ref, (it, pl.ds(0, PAD)))
                clear(mz == counts[2] - 1, ref, (it, pl.ds(PAD, PAD)))
            if not swap:
                clear(mx == 0, xr, (it, 0))
                clear(mx == counts[0] - 1, xr, (it, 1))
                clear(mx == 0, rx, (it, 0))
                clear(mx == counts[0] - 1, rx, (it, 1))

    edges()

    def x_position(slot):
        if swap:
            return jnp.where(slot < nx, slot, slot - jnp.where(mx == 0, 0, nx + PAD))
        return jnp.where(slot < nx, slot, jnp.where(slot < nx + PAD, slot - nx - PAD, slot - PAD))

    def z_position(slot):
        position = jnp.where(slot < PAD, slot - PAD, slot - PAD + nz)
        return jnp.where(slot < 2 * PAD, position, -nz * 4)

    def fill(view, dim, offsets):
        def step(t, total):
            tap = taps_ref[view, dim, t].astype(F32) * (1.0 / 256.0)
            return tuple(jnp.where(o == t, tap, m) for o, m in zip(offsets, total))
        return lax.fori_loop(0, TAPS, step, tuple(jnp.zeros(o.shape, F32) for o in offsets), unroll=4)

    def pair(value, axis):
        return jnp.concatenate([value, value], axis=axis).astype(BF16)

    columns = []
    for v in range(views):
        f_shape, b_shape = (nx, xs), (xs, nx)
        f, b = fill(v, 0, (
            x_position(iota(f_shape, 1)) - iota(f_shape, 0) + REACH,
            x_position(iota(b_shape, 0)) - iota(b_shape, 1) + REACH,
        ))
        kx[pl.ds(v * nx, nx), 0:xs] = f
        kx[pl.ds(v * nx, nx), xs:2 * xs] = f
        columns.append(b)
        f_shape, b_shape = (ny, ys), (ys, ny)
        f, b = fill(v, 1, (
            iota(f_shape, 1) - PAD - iota(f_shape, 0) + REACH,
            iota(b_shape, 0) - PAD - iota(b_shape, 1) + REACH,
        ))
        ky[v] = pair(f, 1)
        kyb[v] = pair(b, 1)
        square = (nz, nz)
        halo = (LANES, nz)
        back = (nz, LANES)
        f, h = fill(v, 2, (
            iota(square, 0) - iota(square, 1) + REACH,
            z_position(iota(halo, 0)) - iota(halo, 1) + REACH,
        ))
        kz[v] = pair(f, 0)
        kzh[v] = pair(h, 0)
        f, b = fill(v, 2, (
            iota(square, 1) - iota(square, 0) + REACH,
            z_position(iota(back, 1)) - iota(back, 0) + REACH,
        ))
        kzb[v, :, 0:nz] = pair(f, 0)
        kzb[v, :, nz:nz + LANES] = pair(b, 0)
    kxb[...] = jnp.concatenate(columns + columns, axis=1).astype(BF16)

    picks = (2 * PAD, LANES)
    ends = jnp.where(iota(picks, 0) < PAD, iota(picks, 0), iota(picks, 0) + nz - 2 * PAD)
    pick_ends = (iota(picks, 1) == ends).astype(F32)
    pick_first = (iota(picks, 1) == iota(picks, 0)).astype(F32)
    ends_wide, first_wide = pair(pick_ends, 1), pair(pick_first, 1)
    ends_tall, first_tall = pair(pick_ends, 0), pair(pick_first, 0)

    normalizer = jnp.float32(0.0)
    for v in range(views):
        product = jnp.float32(1.0)
        for d in range(3):
            total = lax.fori_loop(0, TAPS, lambda t, s, v=v, d=d: s + taps_ref[v, d, t], jnp.int32(0))
            product = product * (total.astype(F32) * (1.0 / 256.0))
        normalizer = normalizer + weights_ref[v].astype(F32) * product

    def loop(low, high, unroll, body):
        assert (high - low) % unroll == 0
        def step(i, carry):
            for u in range(unroll):
                body(low + i * unroll + u)
            return carry
        lax.fori_loop(0, (high - low) // unroll, step, 0)

    def blur_x(source, target, low, high):
        matrix = kx[...].astype(BF16)
        def body(y):
            target[pl.ds(y, views * nx, stride=fstride), :] = dot(matrix, halves(source[y], 0))
        loop(low, high, 4, body)

    def spread_x(source, target):
        matrix = kxb[...]
        weight = scale[...]
        def body(y):
            target[y] = dot(matrix, halves(source[pl.ds(pl.multiple_of(y * ustride, 8), views * nx), :] * weight, 0))
        loop(0, ys, 4, body)

    def turned(source, target, select, it):
        per = LANES // 8
        def body(i):
            block = source[pl.ds(pl.multiple_of(i * LANES, LANES), LANES), :]
            target[it, :, pl.ds(pl.multiple_of(i * LANES, LANES), LANES)] = dot_nt(select, halves(block, 1))
        loop(0, pieces, 4, body)

    for it in range(ITERS):
        last = it == ITERS - 1
        arrive(gathers)
        for y in range(ny):
            for side in range(xr.shape[1]):
                eo[it, PAD + y, pl.ds(nx + side * PAD, PAD), :] = xr[it, side, y]
        gathers = start(y_gather(it))
        blur_x(eo.at[it], fo, PAD, PAD + ny)
        arrive(gathers)
        for y in range(PAD):
            eo[it, y] = yr[it, 0, y]
            eo[it, PAD + ny + y] = yr[it, 1, y]
        turned(eo.at[it].reshape(flat, LANES), ts, ends_wide, it)
        gathers = start(z_pair(it, ts, tr, 4))
        blur_x(eo.at[it], fo, 0, PAD)
        blur_x(eo.at[it], fo, PAD + ny, ys)
        arrive(gathers)
        flat_eh = eh.reshape(flat, LANES)
        def unturn(i):
            at = pl.ds(pl.multiple_of(i * LANES, LANES), LANES)
            flat_eh[at, :] = dot_tn(halves(tr[it, :, at], 0), first_tall)
        loop(0, pieces, 4, unturn)
        blur_x(eh, fh, 0, ys)

        if it == 0:
            image_copy.wait()
        stats[...] = jnp.zeros_like(stats)

        def forward(i, carry):
            v = i // blocks
            base = i * chunk
            own, side = [], []
            for u in range(chunk):
                at = pl.ds(pl.multiple_of((base + u) * fstride, 8), ys)
                both = jnp.concatenate([fo[at, :], fh[at, :]], axis=1)
                value = dot(ky[v], halves(both, 0))
                own.append(value[:, 0:nz])
                side.append(value[:, nz:nz + LANES])
            blurred = dot(halves(jnp.concatenate(own, axis=0), 1), kz[v])
            blurred = blurred + dot(halves(jnp.concatenate(side, axis=0), 1), kzh[v])
            at = pl.ds(pl.multiple_of(i * rows, rows), rows)
            image = img[at, :]
            quo[at, :] = image / blurred
            terms = [blurred, image * blurred, blurred * blurred, image, image * image]
            for k, term in enumerate(terms):
                folded = jnp.sum(term.reshape(rows // 8, 8, nz), axis=0)
                stats[k, v] = stats[k, v] + folded
            return carry

        lax.fori_loop(0, views * blocks, forward, 0)

        def reduce_start(a, value):
            axis, count, me = AXES[a], counts[a], (mx, my, mz)[a]
            ar_own[it, a] = value
            copies = []
            for p in range(1, count):
                c = pltpu.make_async_remote_copy(
                    src_ref=ar_own.at[it, a], dst_ref=ar.at[it, a, p - 1],
                    send_sem=ar_send.at[it, a, p - 1], recv_sem=ar_recv.at[it, a, p - 1],
                    device_id={axis: lax.rem(me + p, count)}, device_id_type=MESH,
                )
                c.start()
                copies.append(c)
            return copies

        def reduce_end(a, copies):
            for c in copies:
                c.wait()
            terms = [ar_own[it, a]] + [ar[it, a, p - 1] for p in range(1, counts[a])]
            while len(terms) > 1:
                half = len(terms) // 2
                terms = [terms[i] + terms[i + half] for i in range(half)] + terms[2 * half:]
            return terms[0]

        def backward(low, high):
            def step(i, carry):
                v = i // blocks
                at = pl.ds(pl.multiple_of(i * rows, rows), rows)
                wide = dot(halves(quo[at, :], 1), kzb[v])
                for u in range(chunk):
                    value = dot(kyb[v], halves(wide[u * ny:(u + 1) * ny], 0))
                    at = pl.ds(i * chunk + u, ys, stride=ustride)
                    uo[at, :] = value[:, 0:nz]
                    uh[at, :] = value[:, nz:nz + LANES]
                return carry
            lax.fori_loop(low, high, step, 0)

        folded = jnp.sum(stats[...], axis=2)
        parts = []
        for k in range(STATS):
            parts += [folded[k], jnp.ones((8 - views, LANES), F32)]
        total = jnp.concatenate(parts, axis=0)
        steps = views * blocks
        marks = (0, steps // 3, 2 * steps // 3, steps)
        for a in range(3):
            copies = reduce_start(a, total)
            backward(marks[a], marks[a + 1])
            total = reduce_end(a, copies)
        total = jnp.broadcast_to(jnp.sum(total, axis=1, keepdims=True), total.shape)
        blurred_total, cross, square, data_total, data_square = (total[8 * k:8 * k + 8] for k in range(STATS))
        flux = data_total / blurred_total
        misfit = (data_square - 2.0 * flux * cross + flux * flux * square) / data_square
        lane = iota(misfit.shape, 1)
        line = jnp.sum(jnp.where(lane == iota(misfit.shape, 0), misfit, 0.0), axis=0, keepdims=True)
        misfit_ref[it:it + 1, :] = line[:, 0:views]
        for v in range(views):
            top = jnp.full((1, LANES), weights_ref[v].astype(F32), F32)
            row = top / (jnp.full((1, LANES), normalizer, F32) * flux[v:v + 1])
            scale[pl.ds(v * nx, nx), :] = jnp.broadcast_to(row, (nx, LANES))

        spread_x(uh, ch)
        turned(ch.reshape(flat, LANES), bs, first_wide, it)
        gathers = start(z_pair(it, bs, br, 6))
        spread_x(uo, co.at[it])
        arrive(gathers)
        flat_co = co.at[it].reshape(flat, LANES)
        def add_z(i):
            at = pl.ds(pl.multiple_of(i * LANES, LANES), LANES)
            flat_co[at, :] = flat_co[at, :] + dot_tn(halves(br[it, :, at], 0), ends_tall)
        loop(0, pieces, 4, add_z)
        gathers = start(y_reduce(it))
        arrive(gathers)
        def add_y(i):
            co[it, PAD + i] = co[it, PAD + i] + ry[it, 0, i]
            co[it, ny + i] = co[it, ny + i] + ry[it, 1, i]
        loop(0, PAD, 4, add_y)
        gathers = start(x_reduce(it))
        arrive(gathers)
        def update(y):
            if swap:
                at = pl.ds(face, PAD)
                co[it, PAD + y, at, :] = co[it, PAD + y, at, :] + rx[it, 0, y]
            else:
                co[it, PAD + y, 0:PAD, :] = co[it, PAD + y, 0:PAD, :] + rx[it, 0, y]
                co[it, PAD + y, nx - PAD:nx, :] = co[it, PAD + y, nx - PAD:nx, :] + rx[it, 1, y]
            value = eo[it, PAD + y, 0:nx, :] * co[it, PAD + y, 0:nx, :]
            if last:
                out_ref[pl.ds(y, nx, stride=ny), :] = value
            else:
                eo[it + 1, PAD + y, 0:nx, :] = value
        loop(0, ny, 4, update)
        if not last:
            gathers = start(x_gather(it + 1))


def local(counts, estimate, view_images, psf_taps, view_weights):
    views, nx, ny, nz = view_images.shape
    sides = 1 if counts[0] == 2 else 2
    xs = nx + sides * PAD
    ys = ny + 2 * PAD
    flat = ys * xs
    vx = views * nx
    peak = max(counts)
    fstride, ustride = ys + 8, vx + 8
    vmem = pltpu.VMEM
    scratch = [
        vmem((views * nx * ny, nz), F32),
        vmem((ITERS, ys, xs, nz), F32),
        vmem((ys, xs, LANES), F32),
        vmem((vx * fstride, nz), F32),
        vmem((vx * fstride, LANES), F32),
        vmem((views * nx * ny, nz), F32),
        vmem((ys * ustride, nz), F32),
        vmem((ys * ustride, LANES), F32),
        vmem((ITERS, ys, xs, nz), F32),
        vmem((ys, xs, LANES), F32),
        vmem((ITERS, 2 * PAD, flat), F32),
        vmem((ITERS, 2 * PAD, flat), F32),
        vmem((ITERS, 2 * PAD, flat), F32),
        vmem((ITERS, 2 * PAD, flat), F32),
        vmem((ITERS, 2, PAD, xs, nz), F32),
        vmem((ITERS, sides, ny, PAD, nz), F32),
        vmem((ITERS, 2, PAD, xs, nz), F32),
        vmem((ITERS, sides, ny, PAD, nz), F32),
        vmem((STATS, views, 8, nz), F32),
        vmem((ITERS, 3, peak, STATS * 8, LANES), F32),
        vmem((ITERS, 3, STATS * 8, LANES), F32),
        vmem((vx, LANES), F32),
        vmem((vx, 2 * xs), F32),
        vmem((xs, 2 * vx), BF16),
        vmem((views, ny, 2 * ys), BF16),
        vmem((views, ys, 2 * ny), BF16),
        vmem((views, 2 * nz, nz), BF16),
        vmem((views, 2 * LANES, nz), BF16),
        vmem((views, 2 * nz, nz + LANES), BF16),
        pltpu.SemaphoreType.DMA(()),
        pltpu.SemaphoreType.DMA((ITERS, 12)),
        pltpu.SemaphoreType.DMA((ITERS, 12)),
        pltpu.SemaphoreType.DMA((ITERS, 3, peak)),
        pltpu.SemaphoreType.DMA((ITERS, 3, peak)),
    ]
    smem = pl.BlockSpec(memory_space=pltpu.SMEM)
    inside = pl.BlockSpec(memory_space=pltpu.VMEM)
    out, misfit = pl.pallas_call(
        functools.partial(kernel, (counts, (views, nx, ny, nz))),
        out_shape=[
            jax.ShapeDtypeStruct((nx * ny, nz), F32),
            jax.ShapeDtypeStruct((ITERS, views), F32),
        ],
        in_specs=[smem, smem, inside, pl.BlockSpec(memory_space=pl.ANY)],
        out_specs=[inside, inside],
        scratch_shapes=scratch,
        compiler_params=pltpu.CompilerParams(
            collective_id=0, has_side_effects=True, vmem_limit_bytes=60 * 1024 * 1024
        ),
    )(psf_taps, view_weights, estimate.reshape(nx * ny, nz), view_images.reshape(views * nx * ny, nz))
    return out.reshape(nx, ny, nz), misfit


def solution(mesh):
    counts = tuple(mesh.shape[a] for a in AXES)
    placed = (P("gx", "gy", "gz"), P(None, "gx", "gy", "gz"), P(), P())
    return jax.shard_map(
        functools.partial(local, counts), mesh=mesh, in_specs=placed,
        out_specs=(P("gx", "gy", "gz"), P()), check_vma=False,
    )
```

```python
import functools

import jax
import jax.numpy as jnp
from jax import lax
from jax.experimental import pallas as pl
from jax.experimental.pallas import tpu as pltpu
from jax.sharding import PartitionSpec as P

TAPS = 31
ITERS = 2
REACH = 15
PAD = 16
LANES = 128
MESH = pl.DeviceIdType.MESH
AXES = ("gx", "gy", "gz")
F32 = jnp.float32
BF16 = jnp.bfloat16
STATS = 5


def halves(value, axis):
    high = value.astype(BF16).astype(F32)
    return jnp.concatenate([high, value - high], axis=axis).astype(BF16)


def dot(left, right):
    return jnp.dot(left, right, preferred_element_type=F32)


def dot_nt(left, right):
    return lax.dot_general(left, right, (((1,), (1,)), ((), ())), preferred_element_type=F32)


def dot_tn(left, right):
    return lax.dot_general(left, right, (((0,), (0,)), ((), ())), preferred_element_type=F32)


def iota(shape, dim):
    return lax.broadcasted_iota(jnp.int32, shape, dim)


class Shift:
    def __init__(self, axis, count, step, source, target, send_sem, recv_sem, swap=False):
        me = lax.axis_index(axis)
        if swap:
            self.sends = self.receives = None
            goal = 1 - me
        else:
            self.sends = (me + step >= 0) & (me + step < count)
            self.receives = (me - step >= 0) & (me - step < count)
            goal = me + step
        self.copy = pltpu.make_async_remote_copy(
            src_ref=source, dst_ref=target, send_sem=send_sem, recv_sem=recv_sem,
            device_id={axis: goal}, device_id_type=MESH,
        )

    def when(self, condition, action):
        if condition is None:
            action()
        else:
            pl.when(condition)(action)

    def start(self):
        self.when(self.sends, self.copy.start)

    def wait_recv(self):
        self.when(self.receives, self.copy.wait_recv)

    def wait_send(self):
        self.when(self.sends, self.copy.wait_send)


def kernel(sizes, taps_ref, weights_ref, est_ref, images_ref, out_ref, misfit_ref,
           img, eo, xr, ya, yb, eho, ehx, eha, ehy, t1, t2, t3, t4, fo, fh, quo, uo, uh,
           ca, cb, cha, chb, ba, bb, ra, rb, rx, stats, ar1, ar2, ar_own, scale,
           kx, kxb, ky, kyb, kz, kzh, kzb, img_sem, send, recv, ar_send, ar_recv):
    counts, (views, nx, ny, nz) = sizes
    swap = counts[0] == 2
    sides = 1 if swap else 2
    xs = nx + sides * PAD
    ys = ny + 2 * PAD
    fstride = fo.shape[0] // (views * nx)
    ustride = uo.shape[0] // ys
    chunk = 8
    rows = chunk * ny
    blocks = nx // chunk
    mx, my, mz = (lax.axis_index(a) for a in AXES)

    image_copy = pltpu.make_async_copy(images_ref, img, img_sem)
    image_copy.start()

    plane = [(p, q) for p in range(counts[0]) for q in range(counts[1]) if p or q]
    barrier = pltpu.get_barrier_semaphore()

    def in_plane(p, q):
        return {"gx": lax.rem(mx + p, counts[0]), "gy": lax.rem(my + q, counts[1])}

    for p, q in plane:
        pl.semaphore_signal(barrier, inc=1, device_id=in_plane(p, q), device_id_type=MESH)
    for p in range(1, counts[2]):
        pl.semaphore_signal(barrier, inc=1, device_id={"gz": lax.rem(mz + p, counts[2])}, device_id_type=MESH)

    for y in range(ny):
        eo[0, y] = est_ref[pl.ds(y, nx, stride=ny), :]

    pl.semaphore_wait(barrier, len(plane) + counts[2] - 1)

    face = pl.multiple_of((1 - mx) * (nx - PAD), 8) if swap else None
    low, high = pl.ds(0, PAD), pl.ds(PAD, PAD)
    tail = pl.ds(ny - PAD, PAD)
    used = [0] * ITERS

    def shift(it, axis, step, source, target, swap=False):
        k = used[it]
        used[it] += 1
        return Shift(axis, counts[AXES.index(axis)], step, source, target, send.at[it, k], recv.at[it, k], swap)

    def start(copies):
        for c in copies:
            c.start()
        return copies

    def arrive(copies):
        for c in copies:
            c.wait_recv()
            c.wait_send()

    def x_gather(it):
        if swap:
            return start([shift(it, "gx", 1, eo.at[it, :, pl.ds(face, PAD), :], xr.at[it, 0], swap=True)])
        return start([
            shift(it, "gx", 1, eo.at[it, :, pl.ds(nx - PAD, PAD), :], xr.at[it, 0]),
            shift(it, "gx", -1, eo.at[it, :, low, :], xr.at[it, 1]),
        ])

    def y_gather(it, source, target):
        return start([
            shift(it, "gy", 1, source.at[tail], target(0)),
            shift(it, "gy", -1, source.at[low], target(1)),
        ])

    def z_pair(it, buffer):
        return start([
            shift(it, "gz", 1, buffer.at[it, 0, high], buffer.at[it, 1, low]),
            shift(it, "gz", -1, buffer.at[it, 0, low], buffer.at[it, 1, high]),
        ])

    def y_reduce(it, source, target):
        return start([
            shift(it, "gy", 1, source.at[pl.ds(PAD + ny, PAD)], target.at[0]),
            shift(it, "gy", -1, source.at[low], target.at[1]),
        ])

    def x_reduce(it):
        own = pl.ds(PAD, ny)
        if swap:
            return start([shift(it, "gx", 1, cb.at[it, 0, own], rx.at[it, 0], swap=True)])
        return start([
            shift(it, "gx", 1, cb.at[it, 1, own], rx.at[it, 0]),
            shift(it, "gx", -1, cb.at[it, 0, own], rx.at[it, 1]),
        ])

    def edges():
        def clear(condition, refs):
            @pl.when(condition)
            def _():
                for ref in refs:
                    ref[...] = jnp.zeros(ref.shape, F32)
        both = range(ITERS)
        for d, edge in ((0, my == 0), (1, my == counts[1] - 1)):
            clear(edge, [r for it in both for r in (ya.at[it, d], yb.at[it, d], ra.at[it, d])]
                  + [rb.at[it, s, d] for it in both for s in range(sides)])
        for part, edge in ((low, mz == 0), (high, mz == counts[2] - 1)):
            clear(edge, [r.at[it, 1, part] for it in both for r in (t1, t2, t3, t4, ba, bb)])
        if not swap:
            for d, edge in ((0, mx == 0), (1, mx == counts[0] - 1)):
                clear(edge, [r.at[it, d] for it in both for r in (xr, rx)])

    def x_position(slot):
        if swap:
            return jnp.where(slot < nx, slot, slot - jnp.where(mx == 0, 0, nx + PAD))
        return jnp.where(slot < nx, slot, jnp.where(slot < nx + PAD, slot - nx - PAD, slot - PAD))

    def z_position(slot):
        position = jnp.where(slot < PAD, slot - PAD, slot - PAD + nz)
        return jnp.where(slot < 2 * PAD, position, -nz * 4)

    def fill(view, dim, offsets):
        def step(t, total):
            tap = taps_ref[view, dim, t].astype(F32) * (1.0 / 256.0)
            return tuple(jnp.where(o == t, tap, m) for o, m in zip(offsets, total))
        return lax.fori_loop(0, TAPS, step, tuple(jnp.zeros(o.shape, F32) for o in offsets), unroll=4)

    def pair(value, axis):
        return jnp.concatenate([value, value], axis=axis).astype(BF16)

    def matrices():
        columns = []
        for v in range(views):
            f_shape, b_shape = (nx, xs), (xs, nx)
            f, b = fill(v, 0, (
                x_position(iota(f_shape, 1)) - iota(f_shape, 0) + REACH,
                x_position(iota(b_shape, 0)) - iota(b_shape, 1) + REACH,
            ))
            kx[pl.ds(v * nx, nx), 0:xs] = f
            kx[pl.ds(v * nx, nx), xs:2 * xs] = f
            columns.append(b)
            f_shape, b_shape = (ny, ys), (ys, ny)
            f, b = fill(v, 1, (
                iota(f_shape, 1) - PAD - iota(f_shape, 0) + REACH,
                iota(b_shape, 0) - PAD - iota(b_shape, 1) + REACH,
            ))
            ky[v] = pair(f, 1)
            kyb[v] = pair(b, 1)
            square = (nz, nz)
            halo = (LANES, nz)
            back = (nz, LANES)
            f, h = fill(v, 2, (
                iota(square, 0) - iota(square, 1) + REACH,
                z_position(iota(halo, 0)) - iota(halo, 1) + REACH,
            ))
            kz[v] = pair(f, 0)
            kzh[v] = pair(h, 0)
            f, b = fill(v, 2, (
                iota(square, 1) - iota(square, 0) + REACH,
                z_position(iota(back, 1)) - iota(back, 0) + REACH,
            ))
            kzb[v, :, 0:nz] = pair(f, 0)
            kzb[v, :, nz:nz + LANES] = pair(b, 0)
        kxb[...] = jnp.concatenate(columns + columns, axis=1).astype(BF16)


    picks = (2 * PAD, LANES)
    ends = jnp.where(iota(picks, 0) < PAD, iota(picks, 0), iota(picks, 0) + nz - 2 * PAD)
    pick_ends = (iota(picks, 1) == ends).astype(F32)
    pick_first = (iota(picks, 1) == iota(picks, 0)).astype(F32)
    ends_wide, first_wide = pair(pick_ends, 1), pair(pick_first, 1)
    ends_tall, first_tall = pair(pick_ends, 0), pair(pick_first, 0)

    normalizer = jnp.float32(0.0)
    for v in range(views):
        product = jnp.float32(1.0)
        for d in range(3):
            total = lax.fori_loop(0, TAPS, lambda t, s, v=v, d=d: s + taps_ref[v, d, t], jnp.int32(0))
            product = product * (total.astype(F32) * (1.0 / 256.0))
        normalizer = normalizer + weights_ref[v].astype(F32) * product

    def loop(count, body, unroll=8):
        unroll = max(u for u in range(1, unroll + 1) if count % u == 0)
        def step(i, carry):
            for u in range(unroll):
                body(i * unroll + u)
            return carry
        if unroll == count:
            step(0, 0)
        else:
            lax.fori_loop(0, count // unroll, step, 0)

    def blur_x(sources, target, count, first):
        matrix = kx[...].astype(BF16)
        def body(y):
            block = jnp.concatenate([r[y] for r in sources], axis=0)
            target[pl.ds(first + y, views * nx, stride=fstride), :] = dot(matrix, halves(block, 0))
        loop(count, body)

    def blur_own(own, beside, target):
        blur_x([own] + [beside.at[s] for s in range(sides)], target, ny, PAD)

    def blur_halo(own, beside, target):
        for d in range(2):
            blur_x([own.at[d]] + [beside.at[d, s] for s in range(sides)], target, PAD, d * (PAD + ny))

    def spread_x(source, target_own, target_side):
        matrix = kxb[...]
        weight = scale[...]
        def body(y):
            value = source[pl.ds(pl.multiple_of(y * ustride, 8), views * nx), :] * weight
            value = dot(matrix, halves(value, 0))
            target_own[y] = value[0:nx]
            for s in range(sides):
                target_side[s, y] = value[nx + s * PAD:nx + (s + 1) * PAD]
        loop(ys, body)

    def flat(ref):
        count = 1
        for d in ref.shape[:-1]:
            count *= d
        return ref.reshape(count, LANES), count // LANES

    def turned(it, source, buffer, select):
        ref, pieces = flat(source)
        def body(i):
            at = pl.ds(pl.multiple_of(i * LANES, LANES), LANES)
            buffer[it, 0, :, at] = dot_nt(select, halves(ref[at, :], 1))
        loop(pieces, body)

    def unturned(it, buffer, select, target, add):
        ref, pieces = flat(target)
        def body(i):
            at = pl.ds(pl.multiple_of(i * LANES, LANES), LANES)
            value = dot_tn(halves(buffer[it, 1, :, at], 0), select)
            ref[at, :] = ref[at, :] + value if add else value
        loop(pieces, body)

    for it in range(ITERS):
        last = it == ITERS - 1
        if it == 0:
            sent_x = x_gather(0)
        sent_y = y_gather(it, eo.at[it], lambda d: ya.at[it, d])
        turned(it, eo.at[it], t1, ends_wide)
        sent_1 = z_pair(it, t1)
        if it == 0:
            edges()
            matrices()
        arrive(sent_y)
        turned(it, ya.at[it], t2, ends_wide)
        sent_2 = z_pair(it, t2)
        arrive(sent_1)
        unturned(it, t1, first_tall, eho, False)
        arrive(sent_x)
        sent_y = []
        for s in range(sides):
            sent_y += y_gather(it, xr.at[it, s], lambda d, s=s: yb.at[it, d, s])
        turned(it, xr.at[it], t3, ends_wide)
        sent_3 = z_pair(it, t3)
        arrive(sent_2)
        unturned(it, t2, first_tall, eha, False)
        blur_own(eo.at[it], xr.at[it], fo)
        arrive(sent_y)
        turned(it, yb.at[it], t4, ends_wide)
        sent_4 = z_pair(it, t4)
        blur_halo(ya.at[it], yb.at[it], fo)
        arrive(sent_3)
        unturned(it, t3, first_tall, ehx, False)
        blur_own(eho, ehx, fh)
        arrive(sent_4)
        unturned(it, t4, first_tall, ehy, False)
        blur_halo(eha, ehy, fh)

        if it == 0:
            image_copy.wait()
        stats[...] = jnp.zeros_like(stats)

        def forward(i, carry):
            v = i // blocks
            base = i * chunk
            own, side = [], []
            for u in range(chunk):
                at = pl.ds(pl.multiple_of((base + u) * fstride, 8), ys)
                both = jnp.concatenate([fo[at, :], fh[at, :]], axis=1)
                value = dot(ky[v], halves(both, 0))
                own.append(value[:, 0:nz])
                side.append(value[:, nz:nz + LANES])
            blurred = dot(halves(jnp.concatenate(own, axis=0), 1), kz[v])
            blurred = blurred + dot(halves(jnp.concatenate(side, axis=0), 1), kzh[v])
            at = pl.ds(pl.multiple_of(i * rows, rows), rows)
            image = img[at, :]
            quo[at, :] = image / blurred
            terms = [blurred, image * blurred, blurred * blurred, image, image * image]
            for k, term in enumerate(terms):
                folded = jnp.sum(term.reshape(rows // 8, 8, nz), axis=0)
                stats[k, v] = stats[k, v] + folded
            return carry

        lax.fori_loop(0, views * blocks, forward, 0, unroll=2)

        def reduce_start(k, value, buffer, peers):
            ar_own[it, k] = value
            copies = []
            for n, peer in enumerate(peers):
                c = pltpu.make_async_remote_copy(
                    src_ref=ar_own.at[it, k], dst_ref=buffer.at[it, n],
                    send_sem=ar_send.at[it, k, n], recv_sem=ar_recv.at[it, k, n],
                    device_id=peer, device_id_type=MESH,
                )
                c.start()
                copies.append(c)
            return copies

        def tree(terms):
            while len(terms) > 1:
                half = len(terms) // 2
                terms = [terms[i] + terms[i + half] for i in range(half)] + terms[2 * half:]
            return terms[0]

        def backward(low, high):
            def step(i, carry):
                v = i // blocks
                at = pl.ds(pl.multiple_of(i * rows, rows), rows)
                wide = dot(halves(quo[at, :], 1), kzb[v])
                for u in range(chunk):
                    value = dot(kyb[v], halves(wide[u * ny:(u + 1) * ny], 0))
                    at = pl.ds(i * chunk + u, ys, stride=ustride)
                    uo[at, :] = value[:, 0:nz]
                    uh[at, :] = value[:, nz:nz + LANES]
                return carry
            lax.fori_loop(low, high, step, 0, unroll=2)

        lane = iota((8, LANES), 1)
        block = jnp.zeros((8, LANES), F32)
        for k in range(STATS):
            sums = jnp.concatenate(
                [jnp.sum(stats[k, v], axis=0, keepdims=True) for v in range(views)]
                + [jnp.ones((8 - views, LANES), F32)], axis=0)
            block = jnp.where(lane == k, jnp.sum(sums, axis=1, keepdims=True), block)
        steps = views * blocks
        copies = reduce_start(0, block, ar1, [in_plane(p, q) for p, q in plane])
        backward(0, steps // 2)
        for c in copies:
            c.wait()
        terms = {pq: ar1[it, n] for n, pq in enumerate(plane)}
        terms[0, 0] = ar_own[it, 0]
        block = tree([tree([terms[p, q] for p in range(counts[0])]) for q in range(counts[1])])
        copies = reduce_start(1, block, ar2, [{"gz": lax.rem(mz + p, counts[2])} for p in range(1, counts[2])])
        backward(steps // 2, steps)
        for c in copies:
            c.wait()
        block = tree([ar_own[it, 1]] + [ar2[it, n] for n in range(counts[2] - 1)])
        blurred_total, cross, square, data_total, data_square = (
            jnp.broadcast_to(block[:, k:k + 1], block.shape) for k in range(STATS))
        flux = data_total / blurred_total
        misfit = (data_square - 2.0 * flux * cross + flux * flux * square) / data_square
        line = jnp.sum(jnp.where(lane == iota(misfit.shape, 0), misfit, 0.0), axis=0, keepdims=True)
        misfit_ref[it:it + 1, :] = line[:, 0:views]
        for v in range(views):
            top = jnp.full((1, LANES), weights_ref[v].astype(F32), F32)
            row = top / (jnp.full((1, LANES), normalizer, F32) * flux[v:v + 1])
            scale[pl.ds(v * nx, nx), :] = jnp.broadcast_to(row, (nx, LANES))

        spread_x(uh, cha, chb)
        turned(it, chb, bb, first_wide)
        sent_b = z_pair(it, bb)
        turned(it, cha, ba, first_wide)
        sent_a = z_pair(it, ba)
        spread_x(uo, ca.at[it], cb.at[it])
        arrive(sent_b)
        unturned(it, bb, ends_tall, cb.at[it], True)
        sent_b = []
        for s in range(sides):
            sent_b += y_reduce(it, cb.at[it, s], rb.at[it, s])
        arrive(sent_a)
        unturned(it, ba, ends_tall, ca.at[it], True)
        sent_a = y_reduce(it, ca.at[it], ra.at[it])
        arrive(sent_b)
        for s in range(sides):
            for y in range(PAD):
                cb[it, s, PAD + y] = cb[it, s, PAD + y] + rb[it, s, 0, y]
                cb[it, s, ny + y] = cb[it, s, ny + y] + rb[it, s, 1, y]
        sent_x = x_reduce(it)
        arrive(sent_a)
        for y in range(PAD):
            ca[it, PAD + y] = ca[it, PAD + y] + ra[it, 0, y]
            ca[it, ny + y] = ca[it, ny + y] + ra[it, 1, y]
        arrive(sent_x)
        for y in range(ny):
            if swap:
                at = pl.ds(face, PAD)
                ca[it, PAD + y, at, :] = ca[it, PAD + y, at, :] + rx[it, 0, y]
            else:
                ca[it, PAD + y, low, :] = ca[it, PAD + y, low, :] + rx[it, 0, y]
                at = pl.ds(nx - PAD, PAD)
                ca[it, PAD + y, at, :] = ca[it, PAD + y, at, :] + rx[it, 1, y]
            value = eo[it, y] * ca[it, PAD + y]
            if last:
                out_ref[pl.ds(y, nx, stride=ny), :] = value
            else:
                eo[it + 1, y] = value
        if not last:
            sent_x = x_gather(it + 1)


def local(counts, estimate, view_images, psf_taps, view_weights):
    views, nx, ny, nz = view_images.shape
    sides = 1 if counts[0] == 2 else 2
    xs = nx + sides * PAD
    ys = ny + 2 * PAD
    vx = views * nx
    peak = max(counts[0] * counts[1], counts[2])
    fstride, ustride = ys + 8, vx + 8
    vmem = pltpu.VMEM
    own_own, own_halo, halo_own, halo_halo = ny * nx, 2 * PAD * nx, sides * ny * PAD, 2 * sides * PAD * PAD
    scratch = [
        vmem((views * nx * ny, nz), F32),
        vmem((ITERS, ny, nx, nz), F32),
        vmem((ITERS, sides, ny, PAD, nz), F32),
        vmem((ITERS, 2, PAD, nx, nz), F32),
        vmem((ITERS, 2, sides, PAD, PAD, nz), F32),
        vmem((ny, nx, LANES), F32),
        vmem((sides, ny, PAD, LANES), F32),
        vmem((2, PAD, nx, LANES), F32),
        vmem((2, sides, PAD, PAD, LANES), F32),
        vmem((ITERS, 2, 2 * PAD, own_own), F32),
        vmem((ITERS, 2, 2 * PAD, own_halo), F32),
        vmem((ITERS, 2, 2 * PAD, halo_own), F32),
        vmem((ITERS, 2, 2 * PAD, halo_halo), F32),
        vmem((vx * fstride, nz), F32),
        vmem((vx * fstride, LANES), F32),
        vmem((views * nx * ny, nz), F32),
        vmem((ys * ustride, nz), F32),
        vmem((ys * ustride, LANES), F32),
        vmem((ITERS, ys, nx, nz), F32),
        vmem((ITERS, sides, ys, PAD, nz), F32),
        vmem((ys, nx, LANES), F32),
        vmem((sides, ys, PAD, LANES), F32),
        vmem((ITERS, 2, 2 * PAD, ys * nx), F32),
        vmem((ITERS, 2, 2 * PAD, sides * ys * PAD), F32),
        vmem((ITERS, 2, PAD, nx, nz), F32),
        vmem((ITERS, sides, 2, PAD, PAD, nz), F32),
        vmem((ITERS, sides, ny, PAD, nz), F32),
        vmem((STATS, views, 8, nz), F32),
        vmem((ITERS, counts[0] * counts[1], 8, LANES), F32),
        vmem((ITERS, counts[2], 8, LANES), F32),
        vmem((ITERS, 2, 8, LANES), F32),
        vmem((vx, LANES), F32),
        vmem((vx, 2 * xs), F32),
        vmem((xs, 2 * vx), BF16),
        vmem((views, ny, 2 * ys), BF16),
        vmem((views, ys, 2 * ny), BF16),
        vmem((views, 2 * nz, nz), BF16),
        vmem((views, 2 * LANES, nz), BF16),
        vmem((views, 2 * nz, nz + LANES), BF16),
        pltpu.SemaphoreType.DMA(()),
        pltpu.SemaphoreType.DMA((ITERS, 32)),
        pltpu.SemaphoreType.DMA((ITERS, 32)),
        pltpu.SemaphoreType.DMA((ITERS, 2, peak)),
        pltpu.SemaphoreType.DMA((ITERS, 2, peak)),
    ]
    smem = pl.BlockSpec(memory_space=pltpu.SMEM)
    inside = pl.BlockSpec(memory_space=pltpu.VMEM)
    out, misfit = pl.pallas_call(
        functools.partial(kernel, (counts, (views, nx, ny, nz))),
        out_shape=[
            jax.ShapeDtypeStruct((nx * ny, nz), F32),
            jax.ShapeDtypeStruct((ITERS, views), F32),
        ],
        in_specs=[smem, smem, inside, pl.BlockSpec(memory_space=pl.ANY)],
        out_specs=[inside, inside],
        scratch_shapes=scratch,
        compiler_params=pltpu.CompilerParams(
            collective_id=0, has_side_effects=True, vmem_limit_bytes=60 * 1024 * 1024
        ),
    )(psf_taps, view_weights, estimate.reshape(nx * ny, nz), view_images.reshape(views * nx * ny, nz))
    return out.reshape(nx, ny, nz), misfit


def solution(mesh):
    counts = tuple(mesh.shape[a] for a in AXES)
    placed = (P("gx", "gy", "gz"), P(None, "gx", "gy", "gz"), P(), P())
    return jax.shard_map(
        functools.partial(local, counts), mesh=mesh, in_specs=placed,
        out_specs=(P("gx", "gy", "gz"), P()), check_vma=False,
    )
```
